32 devices in a mesh: tm: 16 (over z, y, core), asset: 2 (over x).
Axes of the slice: x: 2, y: 2, z: 4, core: 2. Of those that a mesh axis runs over, the one named last changes fastest.
Arguments:
- returns: bfloat16 [64, 8192], P('tm', 'asset'), as said below
- signal: bfloat16 [64, 8192], P('tm', 'asset'), may hold values from -6 to 6
- earlier: bfloat16 [59, 8192], P(None, 'asset'), as said below
Outputs:
- filtered: float32 [64, 8192], P('tm', 'asset')
The draws below stay inside these ranges and needn't reach their ends.
Inputs may be any that keep to these rules, and one draw needn't show every extreme that they name: Each equity has its own scale of returns, the same in returns and earlier. `earlier`: drawn by the same law as returns, with the same scale for each equity.
All inputs are finite; a program needn't handle non-finite values.
Results may differ from the reference program's by a relative error of at most 0.0032.
Values may be sent and summed in bfloat16 or wider, within the bound.
No kernel may reach another device: no remote copies, remote signals or barrier semaphores. Data moves between devices by JAX's collectives and lax.ppermute only.
A program may use at most 64 MiB of HBM per device.

```python
import jax
import jax.numpy as jnp
from jax import lax

ASSETS = 8192
WIN = 60
HIST = 59
DAYS = 64


def asset_scales(key):
    sub_key = jax.random.fold_in(key, 7)
    return jnp.exp(jax.random.uniform(sub_key, (ASSETS,), jnp.float32, jnp.log(0.1), jnp.log(3.0)))


def draw_rows(key, salt, count):
    scales = asset_scales(key)
    noise_key = jax.random.fold_in(key, salt)
    values = jnp.clip(jax.random.normal(noise_key, (count, ASSETS), jnp.float32), -6.0, 6.0)
    return (values * scales[None, :]).astype(jnp.bfloat16)


def draw_returns(key, part):
    return draw_rows(key, 11, DAYS)


def draw_earlier(key, part):
    return draw_rows(key, 13, HIST)


def level_of(own_key, extent, shards, low, largest):
    loudness = 1.0
    for axis_at, shards_of in shards:
        heights = jax.random.uniform(jax.random.fold_in(jax.random.fold_in(own_key, 6), axis_at), (shards_of,), jnp.float32, low / len(shards), largest / len(shards))
        loudness = loudness * jnp.repeat(jnp.exp(heights), extent[axis_at] // shards_of).reshape((-1,) + (1,) * (len(extent) - 1 - axis_at))
    return loudness


def scatter_about(own_key, shape, deviation, bound, shards=(), kind=jnp.bfloat16):
    gain = level_of(own_key, shape, shards, -0.22, 0.18) if shards else 1.0
    drawn = jax.random.normal(own_key, shape, jnp.float32) * deviation * gain
    return jnp.minimum(jnp.maximum(drawn, -bound), bound).astype(kind)


def setup_inputs(seed: int = 0) -> dict:
    keys = jax.random.split(jax.random.key(seed), 4)
    returns = draw_returns(jax.random.fold_in(keys[3], 71), 0)
    signal = scatter_about(keys[1], (DAYS, ASSETS), 1.0, 6.0, ((0, 16), (1, 2)))
    earlier = draw_earlier(jax.random.fold_in(keys[3], 71), 0)
    return {"returns": returns, "signal": signal, "earlier": earlier}


var_floor = 0.05
shrink_level = 0.1

def moments(window):
    values = window.astype(jnp.float32)
    center = lax.optimization_barrier(jnp.mean(values, axis=0))
    spread = lax.optimization_barrier(jnp.mean(values * values, axis=0)) - center * center
    return (center, jnp.sqrt(jnp.maximum(spread, var_floor)))

def contribution(ext_rows, ext_cols, signal_cols):

    def one_day(day_index):
        window_rows = lax.dynamic_slice_in_dim(ext_rows, day_index, WIN, 0)
        window_cols = lax.dynamic_slice_in_dim(ext_cols, day_index, WIN, 0)
        mean_rows, scale_rows = moments(window_rows)
        mean_cols, scale_cols = moments(window_cols)
        gram_tile = lax.dot_general(window_rows, window_cols, (((0,), (0,)), ((), ())), preferred_element_type=jnp.float32)
        correlation = (gram_tile / WIN - mean_rows[:, None] * mean_cols[None, :]) / (scale_rows[:, None] * scale_cols[None, :])
        shrunk = (jnp.sign(correlation) * jnp.maximum(jnp.abs(correlation) - shrink_level, 0.0)).astype(jnp.bfloat16)
        day_signal = lax.dynamic_index_in_dim(signal_cols, day_index, 0, keepdims=False)
        return jnp.dot(shrunk, day_signal, preferred_element_type=jnp.float32)
    return lax.map(one_day, jnp.arange(signal_cols.shape[0], dtype=jnp.int32))

def reference(returns, signal, earlier):
    extended = jnp.concatenate([earlier, returns], 0)
    row_block = min(ASSETS, 1024)
    blocks_count = ASSETS // row_block

    def row_part(block_index):
        own_rows = lax.dynamic_slice_in_dim(extended, block_index * row_block, row_block, 1)
        return contribution(own_rows, extended, signal)
    stacked = lax.map(row_part, jnp.arange(blocks_count, dtype=jnp.int32))
    return jnp.transpose(stacked, (1, 0, 2)).reshape(DAYS, ASSETS)
```

```python
import functools

import jax
import jax.numpy as jnp
from jax import lax
from jax.experimental import pallas as pl
from jax.experimental.pallas import tpu as pltpu
from jax.sharding import PartitionSpec as P

WIN = 60
HIST = 59
SEG = 64
BLK = 512
CHUNK = 32
VAR_FLOOR = 0.05
SHRINK = 0.1
TINY = 1e-30


def history(block_rows, earlier_rows):
    day_dev = block_rows.shape[0]
    position = lax.axis_index("tm")
    span = HIST + day_dev
    all_days = lax.all_gather(block_rows, "tm", axis=0, tiled=True)
    sequence = jnp.concatenate([earlier_rows, all_days], 0)
    return lax.dynamic_slice_in_dim(sequence, position * day_dev, span, 0)


def pair_kernel(tasks, chunks, it_ref, jt_ref, rt_ref, lhs_ref, rhs_ref, sb_ref, b_ref, racc_ref, cacc_ref):
    def body(accs0, accs1):
        racc_ref[...] = jnp.zeros_like(racc_ref)
        cacc_ref[...] = jnp.zeros_like(cacc_ref)

        @pl.when(pl.program_id(0) == 0)
        def _():
            for c in range(chunks):
                pltpu.matmul_pop(accs0[c])
                pltpu.matmul_pop(accs1[c])

        def trip(t, carry):
            now = jnp.minimum(t, tasks - 1)
            i_now = pl.multiple_of(it_ref[now] * BLK, BLK)
            j_now = pl.multiple_of(jt_ref[now] * BLK, BLK)
            old = jnp.maximum(t - 1, 0)
            i_old = pl.multiple_of(it_ref[old] * BLK, BLK)
            j_old = pl.multiple_of(jt_ref[old] * BLK, BLK)
            r_old = pl.multiple_of(rt_ref[old] * BLK, BLK)
            half = BLK // 2
            pltpu.matmul_push_rhs(rhs_ref[0, :, pl.ds(i_now, half)], staging_register=0, mxu_index=0)
            pltpu.matmul_push_rhs(rhs_ref[0, :, pl.ds(i_now + half, half)], staging_register=0, mxu_index=1)
            bound = [b_ref[0, :, pl.ds(i_old + 128 * v, 128)] for v in range(4)]
            low = [-x for x in bound]
            sums = [jnp.zeros((8, 128), jnp.float32) for _ in range(4)]
            for c in range(chunks):
                y0 = pltpu.matmul_pop(accs0[c])
                y1 = pltpu.matmul_pop(accs1[c])
                x = lhs_ref[0, pl.ds(j_now + c * CHUNK, CHUNK), :]
                x = jnp.concatenate([x, x], 1)
                load = 0 if c == 0 else None
                pltpu.matmul_acc_lhs(accs0[c], x, load_staged_rhs=load)
                pltpu.matmul_acc_lhs(accs1[c], x, load_staged_rhs=load)
                for g in range(CHUNK // 8):
                    lo, hi = 8 * g, 8 * g + 8
                    y = [y0[lo:hi, :128], y0[lo:hi, 128:], y1[lo:hi, :128], y1[lo:hi, 128:]]
                    q = [jnp.minimum(jnp.maximum(y[v], low[v]), bound[v]) for v in range(4)]
                    sb = sb_ref[0, pl.ds(j_old + c * CHUNK + lo, 8), :]
                    sums = [sums[v] + q[v] * sb for v in range(4)]
                    rows = pl.ds(r_old + c * CHUNK + lo, 8)
                    racc_ref[0, rows, :] += (q[0] + q[1]) + (q[2] + q[3])
            for v in range(4):
                cacc_ref[0, :, pl.ds(i_old + 128 * v, 128)] += sums[v]
            return carry

        lax.fori_loop(0, tasks + 1, trip, 0)
        for c in range(chunks):
            pltpu.matmul_pop(accs0[c])
            pltpu.matmul_pop(accs1[c])

    specs = [tuple(pltpu.ACC(q)((CHUNK, 256), jnp.float32) for _ in range(chunks)) for q in range(2)]
    pl.run_scoped(body, *specs)


def pair_sums(it, jt, rt, lhs, rhs, sb, b):
    days, rows, _ = lhs.shape
    own = rhs.shape[2]
    tasks = it.shape[0]
    block = lambda *shape: pl.BlockSpec((1,) + shape, lambda d, *_: (d,) + (0,) * len(shape))
    return pl.pallas_call(
        functools.partial(pair_kernel, tasks, BLK // CHUNK),
        grid_spec=pltpu.PrefetchScalarGridSpec(
            num_scalar_prefetch=3,
            grid=(days,),
            in_specs=[block(rows, 128), block(256, own), block(rows, 128), block(8, own)],
            out_specs=[block(rows + BLK, 128), block(8, own)],
        ),
        out_shape=[
            jax.ShapeDtypeStruct((days, rows + BLK, 128), jnp.float32),
            jax.ShapeDtypeStruct((days, 8, own), jnp.float32),
        ],
        compiler_params=pltpu.CompilerParams(vmem_limit_bytes=60 * 1024 * 1024),
        cost_estimate=pl.CostEstimate(
            flops=2 * days * tasks * BLK * BLK * 256, bytes_accessed=days * rows * 128 * 10, transcendentals=0
        ),
    )(it, jt, rt, lhs, rhs, sb, b)


def per_device(shards, returns, signal, earlier):
    day_dev, own = returns.shape
    me = lax.axis_index("asset")
    half = shards // 2
    extended = history(returns, earlier)
    ext, sig = [extended], [signal]
    for s in range(1, half + 1):
        perm = [((p + s) % shards, p) for p in range(shards)]
        ext.append(lax.ppermute(extended, "asset", perm))
        sig.append(lax.ppermute(signal, "asset", perm))
    ext = jnp.concatenate(ext, 1).astype(jnp.float32)
    sig = jnp.concatenate(sig, 1).astype(jnp.float32)
    span = ext.shape[0]
    ext = jnp.pad(ext, ((0, SEG - span), (0, 0)))
    k = lax.broadcasted_iota(jnp.int32, (day_dev, SEG, 1), 1)
    d = lax.broadcasted_iota(jnp.int32, (day_dev, SEG, 1), 0)
    mask = ((k >= d) & (k < d + WIN)).astype(jnp.float32)
    win = ext[None] * mask
    mean = jnp.sum(win, 1, keepdims=True) / WIN
    spread = jnp.sum(win * win, 1, keepdims=True) / WIN - mean * mean
    scale = jnp.sqrt(jnp.maximum(spread, VAR_FLOOR))
    z = (win - mean) * mask / (scale * (WIN**0.5))
    zh = lax.reduce_precision(z, 8, 7)
    zl = z - zh
    lhs = jnp.concatenate([zh, zl], 1).astype(jnp.bfloat16).transpose(0, 2, 1)
    a = sig[:, :own]
    a = jnp.where(jnp.abs(a) < TINY, TINY, a)
    u = z[:, :, :own] * a[:, None, :]
    uh = lax.reduce_precision(u, 8, 7)
    ul = u - uh
    rhs = jnp.concatenate([uh, uh, ul, ul], 1).astype(jnp.bfloat16)
    sb = jnp.broadcast_to(sig[:, :, None], sig.shape + (128,))
    b = jnp.broadcast_to((SHRINK * jnp.abs(a))[:, None, :], (day_dev, 8, own))

    blocks = own // BLK
    reach = blocks * shards // 2
    i_list = [i for i in range(blocks) for _ in range(reach)] + [0] * (blocks // 2)
    j_list = [i + x for i in range(blocks) for x in range(reach)] + [0] * (blocks // 2)
    dummy = (half + 1) * blocks
    r_list = [dummy if x == 0 else i + x for i in range(blocks) for x in range(reach)] + [0] * (blocks // 2)
    far = jnp.arange(blocks // 2, dtype=jnp.int32) + jnp.where(me >= half, blocks // 2, 0)
    body = blocks * reach
    it = jnp.array(i_list, jnp.int32).at[body:].set(far)
    jt = jnp.array(j_list, jnp.int32).at[body:].set(far + reach)
    rt = jnp.array(r_list, jnp.int32).at[body:].set(far + reach)
    racc, cacc = pair_sums(it, jt, rt, lhs, rhs, sb, b)
    row = jnp.sum(racc, 2)
    v = jnp.sum(z * sig[:, None, :], 2, keepdims=True)
    missing = []
    if half > 0 and shards > 2:
        for s in range(half + 1, shards):
            perm = [((p + s) % shards, p) for p in range(shards)]
            missing.append(perm)
    v_own = jnp.sum(z[:, :, :own] * sig[:, None, :own], 2)
    v = lax.psum(v_own, "asset")[:, :, None]
    out = jnp.sum(z[:, :, :own] * v, 1) - jnp.sum(cacc, 1) / a - row[:, :own]
    for s in range(1, half + 1):
        perm = [(p, (p + s) % shards) for p in range(shards)]
        out = out - lax.ppermute(row[:, s * own : (s + 1) * own], "asset", perm)
    return out


def solution(mesh):
    shards = mesh.shape["asset"]
    in_specs = (P("tm", "asset"), P("tm", "asset"), P(None, "asset"))
    return jax.shard_map(
        functools.partial(per_device, shards), mesh=mesh, in_specs=in_specs, out_specs=P("tm", "asset"), check_vma=False
    )
```
